128 devices in a mesh: rows: 2 (over y_hi), cols: 8 (over z, y_lo), slabs: 8 (over x, core).
Axes of the slice: x: 4, y: 4 (y_hi: 2, y_lo: 2; y = y_hi * 2 + y_lo), z: 4, core: 2. Of those that a mesh axis runs over, the one named last changes fastest.
Arguments:
- field_values: float32 [8, 512, 512, 128], P('rows', 'cols', 'slabs'), may hold values from 0.2 to 1.8
- mobility: float32 [8, 512, 512, 128], P('rows', 'cols', 'slabs'), may hold values from 0.03 to 0.15
- source: float32 [8, 512, 512, 128], P('rows', 'cols', 'slabs'), may hold values from -0.2 to 0.2
Outputs:
- column_sum: float32 [8, 512, 512, 128], P('rows', 'cols', 'slabs')
- field_values_end: float32 [8, 512, 512, 128], P('rows', 'cols', 'slabs')
The draws below stay inside these ranges and needn't reach their ends.
All inputs are finite; a program needn't handle non-finite values.
Results may differ from the reference program's by a relative error of at most 0.00002.
Values sent between devices are 32-bit elements; how exact they have to be, the bound alone decides.
A program may use at most 320 MiB of HBM per device.

```python
import jax
import jax.numpy as jnp
from jax import lax

GRID_J = 8
GRID_I = 512
GRID_K = 512
MEMBERS = 128
STEPS = 4


def shard_levels(stream_key, shape, split, low, top_value):
    gain = 1.0
    for position, shards_of in split:
        steps = jax.random.uniform(jax.random.fold_in(jax.random.fold_in(stream_key, 6), position), (shards_of,), jnp.float32, low / len(split), top_value / len(split))
        gain = gain * jnp.repeat(jnp.exp(steps), shape[position] // shards_of).reshape((-1,) + (1,) * (len(shape) - 1 - position))
    return gain


def setup_inputs(seed: int = 0) -> dict:
    streams_of = jax.random.split(jax.random.key(seed), 4)
    return {
        "field_values": jnp.clip(0.2 + 1.5999999 * jax.random.uniform(streams_of[0], (GRID_J, GRID_I, GRID_K, MEMBERS), jnp.float32) ** shard_levels(streams_of[0], (GRID_J, GRID_I, GRID_K, MEMBERS), ((0, 2), (1, 8), (2, 8)), -0.2, 0.2), 0.2, 1.8),
        "mobility": jnp.clip(0.03 + 0.120000007 * jax.random.uniform(streams_of[1], (GRID_J, GRID_I, GRID_K, MEMBERS), jnp.float32) ** shard_levels(streams_of[1], (GRID_J, GRID_I, GRID_K, MEMBERS), ((0, 2), (1, 8), (2, 8)), -0.2, 0.2), 0.03, 0.15),
        "source": jnp.clip(jax.random.uniform(streams_of[2], (GRID_J, GRID_I, GRID_K, MEMBERS), jnp.float32, -0.2, 0.2) * shard_levels(streams_of[2], (GRID_J, GRID_I, GRID_K, MEMBERS), ((0, 2), (1, 8), (2, 8)), -0.4, 0.0), -0.2, 0.2),
    }


def strip_edges(values, dims):
    for dim in dims:
        values = lax.slice_in_dim(values, 1, values.shape[dim] - 1, axis=dim)
    return values


def neighbour(values, dim, start, dims):
    others = [other for other in dims if other != dim]
    values = strip_edges(values, others)
    return lax.slice_in_dim(values, start, start + values.shape[dim] - 2, axis=dim)


def one_step(padded, mobility, source):
    middle = strip_edges(padded, (0, 1, 2))
    lower = [neighbour(padded, dim, 0, (0, 1, 2)) for dim in (0, 1, 2)]
    upper = [neighbour(padded, dim, 2, (0, 1, 2)) for dim in (0, 1, 2)]
    spread = lower[0] + upper[0] + lower[1] + upper[1] + lower[2] + upper[2] - 6.0 * middle
    return middle + mobility * spread + source


def reference(field_values, mobility, source):
    for step in range(STEPS):
        field_values = one_step(jnp.pad(field_values, ((1, 1), (1, 1), (1, 1), (0, 0)), mode="constant"), mobility, source)
    column_sum = jnp.cumsum(field_values, axis=0) / GRID_J
    return column_sum, field_values
```

```python
import functools

import jax
import jax.numpy as jnp
from jax import lax
from jax.experimental import pallas as pl
from jax.experimental.pallas import tpu as pltpu
from jax.sharding import PartitionSpec as P

STEPS = 4
CHUNKS = 8
MESH = pl.DeviceIdType.MESH


def kernel(dims, sizes, f_hbm, m_hbm, s_hbm, cs_hbm, fe_hbm, F, M, S, R, T, KS, KR,
           ld_sem, e_send, e_recv, h_send, h_recv, k_send, k_recv, out_sem):
    J, I, K, L = dims
    n_rows, n_cols, n_slabs = sizes
    W = I // CHUNKS
    r = lax.axis_index("rows")
    c = lax.axis_index("cols")
    s = lax.axis_index("slabs")
    other = 1 - r
    edge = (J - 1) * (1 - r)
    edge_in = (J - 2) * (1 - r) + r
    far = (J - 1) * r
    far_in = (1 - r) + (J - 2) * r
    has_low, has_high = c > 0, c < n_cols - 1
    has_front, has_back = s > 0, s < n_slabs - 1

    def rows_of(chunk, extra=0):
        return pl.ds(chunk * W + extra, W)

    def e_copy(t, chunk):
        if t == 0:
            src = f_hbm.at[edge, rows_of(chunk)]
        elif t < STEPS:
            src = F.at[t % 2, edge, rows_of(chunk, 1)]
        else:
            src = T.at[rows_of(chunk)]
        return pltpu.make_async_remote_copy(
            src_ref=src, dst_ref=R.at[t, rows_of(chunk)],
            send_sem=e_send.at[t, chunk], recv_sem=e_recv.at[t, chunk],
            device_id={"rows": other}, device_id_type=MESH)

    def h_copy(t, up):
        row = I - 1 if up else 0
        src = f_hbm.at[:, row] if t == 0 else F.at[t % 2, :, row + 1]
        return pltpu.make_async_remote_copy(
            src_ref=src, dst_ref=F.at[t % 2, :, 0 if up else I + 1],
            send_sem=h_send.at[t, up], recv_sem=h_recv.at[t, up],
            device_id={"cols": c + 1 if up else c - 1}, device_id_type=MESH)

    def k_copy(t, up, chunk):
        return pltpu.make_async_remote_copy(
            src_ref=KS.at[t, up, :, rows_of(chunk)], dst_ref=KR.at[t, up, :, rows_of(chunk)],
            send_sem=k_send.at[t, up, chunk], recv_sem=k_recv.at[t, up, chunk],
            device_id={"slabs": s + 1 if up else s - 1}, device_id_type=MESH)

    def load(which, chunk):
        hbm = (f_hbm, m_hbm, s_hbm)[which]
        dst = (F.at[0, :, rows_of(chunk, 1)], M.at[:, rows_of(chunk)], S.at[:, rows_of(chunk)])[which]
        return pltpu.make_async_copy(hbm.at[:, rows_of(chunk)], dst, ld_sem.at[which, chunk])

    def put(which, chunk):
        src = (M.at[:, rows_of(chunk)], F.at[STEPS % 2, :, rows_of(chunk, 1)])[which]
        dst = (cs_hbm, fe_hbm)[which]
        return pltpu.make_async_copy(src, dst.at[:, rows_of(chunk)], out_sem.at[which, chunk])

    def loop(n, body):
        def step(i, carry):
            body(i)
            return carry
        lax.fori_loop(0, n, step, 0)

    def chunk_at(pos):
        return (pos + CHUNKS - 1) % CHUNKS

    barrier = pltpu.get_barrier_semaphore()
    greet = [(None, {"rows": other}), (has_low, {"cols": c - 1}), (has_high, {"cols": c + 1}),
             (has_front, {"slabs": s - 1}), (has_back, {"slabs": s + 1})]
    for cond, target in greet:
        def signal(target=target):
            pl.semaphore_signal(barrier, inc=1, device_id=target, device_id_type=MESH)
        signal() if cond is None else pl.when(cond)(signal)
    loop(CHUNKS, lambda i: load(0, i).start())
    peers = (1 + (c + n_cols - 1) // n_cols + (2 * n_cols - 2 - c) // n_cols
             + (s + n_slabs - 1) // n_slabs + (2 * n_slabs - 2 - s) // n_slabs)
    pl.semaphore_wait(barrier, peers)

    pl.when(has_high)(lambda: h_copy(0, 1).start())
    e_copy(0, CHUNKS - 1).start()
    pl.when(has_low)(lambda: h_copy(0, 0).start())
    loop(CHUNKS - 1, lambda i: e_copy(0, i).start())
    for which in (1, 2):
        loop(CHUNKS, lambda i: load(which, i).start())

    zero_row = jnp.zeros((K, L), jnp.float32)
    for cond, row in ((c == 0, 0), (c == n_cols - 1, I + 1)):
        @pl.when(cond)
        def _():
            for slot in range(2):
                for p in range(J):
                    F[slot, p, row] = zero_row
    for cond, up in ((s == 0, 1), (s == n_slabs - 1, 0)):
        @pl.when(cond)
        def _():
            def clear(t):
                for p in range(J):
                    KR[t, up, p] = jnp.zeros((I, L), jnp.float32)
            loop(STEPS, clear)

    def send_faces(t, chunk):
        pl.when(has_front)(lambda: k_copy(t, 0, chunk).start())
        pl.when(has_back)(lambda: k_copy(t, 1, chunk).start())

    loop(CHUNKS, lambda i: load(0, i).wait())

    def first_faces(pos):
        chunk = chunk_at(pos)
        for p in range(J):
            def one(i, p=p):
                row = chunk * W + i
                x = F[0, p, row + 1]
                KS[0, 0, p, pl.ds(row, 1), :] = x[0:1]
                KS[0, 1, p, pl.ds(row, 1), :] = x[K - 1:K]
            loop(W, one)
        send_faces(0, chunk)
    loop(CHUNKS, first_faces)

    k_index = lax.broadcasted_iota(jnp.int32, (K, L), 0)

    def stencil_row(t, p, row, near):
        now, later = t % 2, (t + 1) % 2
        x = F[now, p, row + 1]
        below = jnp.where(k_index == 0, KR[t, 1, p, pl.ds(row, 1), :], pltpu.roll(x, 1, 0))
        above = jnp.where(k_index == K - 1, KR[t, 0, p, pl.ds(row, 1), :], pltpu.roll(x, K - 1, 0))
        total = near(row) + (F[now, p, row] + F[now, p, row + 2]) + (below + above) - 6.0 * x
        y = x + M[p, row] * total + S[p, row]
        F[later, p, row + 1] = y
        if t < STEPS - 1:
            KS[t + 1, 0, p, pl.ds(row, 1), :] = y[0:1]
            KS[t + 1, 1, p, pl.ds(row, 1), :] = y[K - 1:K]

    def step_chunk(t, chunk):
        now = t % 2
        if t == 0:
            load(1, chunk).wait()
            load(2, chunk).wait()
        first, last = chunk == 0, chunk == CHUNKS - 1
        pl.when(has_front)(lambda: k_copy(t, 1, chunk).wait_recv())
        pl.when(has_back)(lambda: k_copy(t, 0, chunk).wait_recv())
        pl.when(first & has_low)(lambda: h_copy(t, 1).wait_recv())
        pl.when(last & has_high)(lambda: h_copy(t, 0).wait_recv())
        if t > 0:
            pl.when(first & has_low)(lambda: h_copy(t - 1, 0).wait_send())
            pl.when(last & has_high)(lambda: h_copy(t - 1, 1).wait_send())
            e_copy(t - 1, chunk).wait_send()
        e_copy(t, chunk).wait_recv()
        base = chunk * W
        loop(W, lambda i: stencil_row(
            t, edge, base + i, lambda row: F[now, edge_in, row + 1] + R[t, row]))
        if t < STEPS - 1:
            e_copy(t + 1, chunk).start()
        loop(W, lambda i: stencil_row(
            t, far, base + i, lambda row: F[now, far_in, row + 1]))
        for p in range(1, J - 1):
            loop(W, lambda i, p=p: stencil_row(
                t, p, base + i, lambda row: F[now, p - 1, row + 1] + F[now, p + 1, row + 1]))
        if t < STEPS - 1:
            pl.when(first & has_low)(lambda: h_copy(t + 1, 0).start())
            pl.when(last & has_high)(lambda: h_copy(t + 1, 1).start())
            send_faces(t + 1, chunk)
        else:
            put(1, chunk).start()

            @pl.when(r == 0)
            def _():
                def totals(i):
                    row = base + i
                    total = F[STEPS % 2, 0, row + 1]
                    M[0, row] = total * (1.0 / (J * n_rows))
                    for p in range(1, J):
                        total = total + F[STEPS % 2, p, row + 1]
                        M[p, row] = total * (1.0 / (J * n_rows))
                    T[row] = total
                loop(W, totals)
                e_copy(STEPS, chunk).start()
                put(0, chunk).start()

    for t in range(STEPS):
        loop(CHUNKS, lambda pos, t=t: step_chunk(t, chunk_at(pos)))

    @pl.when(r == 1)
    def _():
        def finish(pos):
            chunk = chunk_at(pos)
            e_copy(STEPS, chunk).wait_recv()

            def sums(i):
                row = chunk * W + i
                total = R[STEPS, row]
                for p in range(J):
                    total = total + F[STEPS % 2, p, row + 1]
                    M[p, row] = total * (1.0 / (J * n_rows))
            loop(W, sums)
            put(0, chunk).start()
        loop(CHUNKS, finish)

    pl.when(has_low)(lambda: h_copy(STEPS - 1, 0).wait_send())
    pl.when(has_high)(lambda: h_copy(STEPS - 1, 1).wait_send())

    def drain(i):
        e_copy(STEPS - 1, i).wait_send()
        pl.when(r == 0)(lambda: e_copy(STEPS, i).wait_send())
        for t in range(STEPS):
            pl.when(has_front)(lambda t=t: k_copy(t, 0, i).wait_send())
            pl.when(has_back)(lambda t=t: k_copy(t, 1, i).wait_send())
        put(0, i).wait()
        put(1, i).wait()
    loop(CHUNKS, drain)


def local(sizes, field_values, mobility, source):
    J, I, K, L = field_values.shape
    f32 = jnp.float32
    any_space = pl.BlockSpec(memory_space=pl.ANY)
    dma = pltpu.SemaphoreType.DMA
    return tuple(pl.pallas_call(
        functools.partial(kernel, (J, I, K, L), sizes),
        out_shape=[jax.ShapeDtypeStruct((J, I, K, L), f32)] * 2,
        in_specs=[any_space] * 3,
        out_specs=[any_space] * 2,
        scratch_shapes=[
            pltpu.VMEM((2, J, I + 2, K, L), f32),
            pltpu.VMEM((J, I, K, L), f32),
            pltpu.VMEM((J, I, K, L), f32),
            pltpu.VMEM((STEPS + 1, I, K, L), f32),
            pltpu.VMEM((I, K, L), f32),
            pltpu.VMEM((STEPS, 2, J, I, L), f32),
            pltpu.VMEM((STEPS, 2, J, I, L), f32),
            dma((3, CHUNKS)),
            dma((STEPS + 1, CHUNKS)),
            dma((STEPS + 1, CHUNKS)),
            dma((STEPS, 2)),
            dma((STEPS, 2)),
            dma((STEPS, 2, CHUNKS)),
            dma((STEPS, 2, CHUNKS)),
            dma((2, CHUNKS)),
        ],
        compiler_params=pltpu.CompilerParams(
            collective_id=0, has_side_effects=True, vmem_limit_bytes=60 * 1024 * 1024),
        name="diffuse",
    )(field_values, mobility, source))


def solution(mesh):
    spec = P("rows", "cols", "slabs", None)
    sizes = tuple(mesh.shape[axis] for axis in ("rows", "cols", "slabs"))
    return jax.shard_map(functools.partial(local, sizes), mesh=mesh,
                         in_specs=(spec,) * 3, out_specs=(spec,) * 2, check_vma=False)
```

```python
import functools

import jax
import jax.numpy as jnp
from jax import lax
from jax.experimental import pallas as pl
from jax.experimental.pallas import tpu as pltpu
from jax.sharding import PartitionSpec as P

STEPS = 4
CHUNKS = 16
FIRST = 6
AHEAD = 8
MESH = pl.DeviceIdType.MESH


def kernel(dims, sizes, f_hbm, m_hbm, s_hbm, M, S, F, R, T, KS, KR,
           ld_sem, e_send, e_recv, h_send, h_recv, k_send, k_recv):
    J, I, K, L = dims
    n_rows, n_cols, n_slabs = sizes
    W = I // CHUNKS
    r = lax.axis_index("rows")
    c = lax.axis_index("cols")
    s = lax.axis_index("slabs")
    other = 1 - r
    edge = (J - 1) * (1 - r)
    edge_in = (J - 2) * (1 - r) + r
    far = (J - 1) * r
    far_in = (1 - r) + (J - 2) * r
    has_low, has_high = c > 0, c < n_cols - 1
    has_front, has_back = s > 0, s < n_slabs - 1

    def rows_of(chunk, extra=0):
        return pl.ds(chunk * W + extra, W)

    def chunk_at(pos):
        return (pos + FIRST) % CHUNKS

    def edge_rows(t, chunk):
        if t == 0:
            return f_hbm.at[edge, rows_of(chunk)]
        if t < STEPS:
            return F.at[t % 2, edge, rows_of(chunk, 1)]
        return T.at[rows_of(chunk)]

    def e_copy(t, pos):
        chunk = chunk_at(pos)
        return pltpu.make_async_remote_copy(
            src_ref=edge_rows(t, chunk), dst_ref=R.at[t % 2, rows_of(chunk)],
            send_sem=e_send.at[t % 2, pos], recv_sem=e_recv.at[t % 2, pos],
            device_id={"rows": other}, device_id_type=MESH)

    def h_copy(t, up):
        row = I - 1 if up else 0
        src = f_hbm.at[:, row] if t == 0 else F.at[t % 2, :, row + 1]
        return pltpu.make_async_remote_copy(
            src_ref=src, dst_ref=F.at[t % 2, :, 0 if up else I + 1],
            send_sem=h_send.at[t, up], recv_sem=h_recv.at[t, up],
            device_id={"cols": c + 1 if up else c - 1}, device_id_type=MESH)

    def k_copy(t, up, pos):
        chunk = chunk_at(pos)
        return pltpu.make_async_remote_copy(
            src_ref=KS.at[t % 2, up, :, rows_of(chunk)], dst_ref=KR.at[t % 2, up, :, rows_of(chunk)],
            send_sem=k_send.at[t % 2, up, pos], recv_sem=k_recv.at[t % 2, up, pos],
            device_id={"slabs": s + 1 if up else s - 1}, device_id_type=MESH)

    def load(which, pos):
        chunk = chunk_at(pos)
        hbm = (f_hbm, m_hbm, s_hbm)[which]
        dst = (F.at[0, :, rows_of(chunk, 1)], M.at[:, rows_of(chunk)], S.at[:, rows_of(chunk)])[which]
        return pltpu.make_async_copy(hbm.at[:, rows_of(chunk)], dst, ld_sem.at[which, pos])

    def loop(n, body):
        def step(i, carry):
            body(i)
            return carry
        lax.fori_loop(0, n, step, 0)

    def send(t, pos):
        e_copy(t, pos).start()

    barrier = pltpu.get_barrier_semaphore()
    greet = [(None, {"rows": other}), (has_low, {"cols": c - 1}), (has_high, {"cols": c + 1}),
             (has_front, {"slabs": s - 1}), (has_back, {"slabs": s + 1})]
    for cond, target in greet:
        def signal(target=target):
            pl.semaphore_signal(barrier, inc=1, device_id=target, device_id_type=MESH)
        signal() if cond is None else pl.when(cond)(signal)
    loop(CHUNKS, lambda i: load(0, i).start())
    peers = (1 + (c + n_cols - 1) // n_cols + (2 * n_cols - 2 - c) // n_cols
             + (s + n_slabs - 1) // n_slabs + (2 * n_slabs - 2 - s) // n_slabs)
    pl.semaphore_wait(barrier, peers)

    loop(AHEAD, lambda i: send(0, i))

    pl.when(has_high)(lambda: h_copy(0, 1).start())
    pl.when(has_low)(lambda: h_copy(0, 0).start())
    for which in (1, 2):
        loop(CHUNKS, lambda i: load(which, i).start())

    zero_row = jnp.zeros((K, L), jnp.float32)
    for cond, row in ((c == 0, 0), (c == n_cols - 1, I + 1)):
        @pl.when(cond)
        def _():
            for slot in range(2):
                for p in range(J):
                    F[slot, p, row] = zero_row
    for cond, up in ((s == 0, 1), (s == n_slabs - 1, 0)):
        @pl.when(cond)
        def _():
            for slot in range(2):
                for p in range(J):
                    KR[slot, up, p] = jnp.zeros((I, L), jnp.float32)

    def send_faces(t, pos):
        pl.when(has_front)(lambda: k_copy(t, 0, pos).start())
        pl.when(has_back)(lambda: k_copy(t, 1, pos).start())

    loop(CHUNKS, lambda i: load(0, i).wait())

    def first_faces(pos):
        chunk = chunk_at(pos)
        for p in range(J):
            def one(i, p=p):
                row = chunk * W + i
                x = F[0, p, row + 1]
                KS[0, 0, p, pl.ds(row, 1), :] = x[0:1]
                KS[0, 1, p, pl.ds(row, 1), :] = x[K - 1:K]
            loop(W, one)
        send_faces(0, pos)
    loop(CHUNKS, first_faces)

    k_index = lax.broadcasted_iota(jnp.int32, (K, L), 0)

    def stencil_row(t, p, row, near):
        now, later = t % 2, (t + 1) % 2
        x = F[now, p, row + 1]
        below = jnp.where(k_index == 0, KR[now, 1, p, pl.ds(row, 1), :], pltpu.roll(x, 1, 0))
        above = jnp.where(k_index == K - 1, KR[now, 0, p, pl.ds(row, 1), :], pltpu.roll(x, K - 1, 0))
        total = near(row) + (F[now, p, row] + F[now, p, row + 2]) + (below + above) - 6.0 * x
        y = x + M[p, row] * total + S[p, row]
        if t == STEPS - 1:
            S[p, row] = y
        else:
            F[later, p, row + 1] = y
        if t < STEPS - 1:
            KS[later, 0, p, pl.ds(row, 1), :] = y[0:1]
            KS[later, 1, p, pl.ds(row, 1), :] = y[K - 1:K]

    def step_chunk(t, pos):
        now = t % 2
        chunk = chunk_at(pos)
        if t == 0:
            load(1, pos).wait()
            load(2, pos).wait()
        first, last = chunk == 0, chunk == CHUNKS - 1
        e_copy(t, pos).wait_recv()
        pl.when(pos < CHUNKS - AHEAD)(lambda: send(t, pos + AHEAD))
        late = pos >= CHUNKS - AHEAD
        if t == STEPS - 1:
            late = late & (r == 0)
        pl.when(late)(lambda: send(t + 1, pos + AHEAD - CHUNKS))
        pl.when(has_front)(lambda: k_copy(t, 1, pos).wait_recv())
        pl.when(has_back)(lambda: k_copy(t, 0, pos).wait_recv())
        pl.when(first & has_low)(lambda: h_copy(t, 1).wait_recv())
        pl.when(last & has_high)(lambda: h_copy(t, 0).wait_recv())
        if t > 0:
            pl.when(first & has_low)(lambda: h_copy(t - 1, 0).wait_send())
            pl.when(last & has_high)(lambda: h_copy(t - 1, 1).wait_send())
            pl.when(has_front)(lambda: k_copy(t - 1, 0, pos).wait_send())
            pl.when(has_back)(lambda: k_copy(t - 1, 1, pos).wait_send())
            e_copy(t - 1, pos).wait_send()
        base = chunk * W
        loop(W, lambda i: stencil_row(
            t, edge, base + i, lambda row: F[now, edge_in, row + 1] + R[now, row]))
        loop(W, lambda i: stencil_row(
            t, far, base + i, lambda row: F[now, far_in, row + 1]))
        for p in range(1, J - 1):
            loop(W, lambda i, p=p: stencil_row(
                t, p, base + i, lambda row: F[now, p - 1, row + 1] + F[now, p + 1, row + 1]))
        if t < STEPS - 1:
            pl.when(first & has_low)(lambda: h_copy(t + 1, 0).start())
            pl.when(last & has_high)(lambda: h_copy(t + 1, 1).start())
            send_faces(t + 1, pos)
        else:
            @pl.when(r == 0)
            def _():
                def totals(i):
                    row = base + i
                    total = S[0, row]
                    M[0, row] = total * (1.0 / (J * n_rows))
                    for p in range(1, J):
                        total = total + S[p, row]
                        M[p, row] = total * (1.0 / (J * n_rows))
                    T[row] = total
                loop(W, totals)

    for t in range(STEPS):
        loop(CHUNKS, lambda pos, t=t: step_chunk(t, pos))

    @pl.when(r == 0)
    def _():
        loop(CHUNKS - AHEAD, lambda i: send(STEPS, i + AHEAD))

    @pl.when(r == 1)
    def _():
        def finish(pos):
            e_copy(STEPS, pos).wait_recv()

            def sums(i):
                row = chunk_at(pos) * W + i
                total = R[STEPS % 2, row]
                for p in range(J):
                    total = total + S[p, row]
                    M[p, row] = total * (1.0 / (J * n_rows))
            loop(W, sums)
        loop(CHUNKS, finish)

    pl.when(has_low)(lambda: h_copy(STEPS - 1, 0).wait_send())
    pl.when(has_high)(lambda: h_copy(STEPS - 1, 1).wait_send())

    def drain(i):
        e_copy(STEPS - 1, i).wait_send()
        pl.when(r == 0)(lambda: e_copy(STEPS, i).wait_send())
        pl.when(has_front)(lambda: k_copy(STEPS - 1, 0, i).wait_send())
        pl.when(has_back)(lambda: k_copy(STEPS - 1, 1, i).wait_send())
    loop(CHUNKS, drain)


def write_out(cs_vmem, fe_vmem, cs_hbm, fe_hbm, sem):
    W = cs_vmem.shape[1] // CHUNKS

    def put(which, i):
        src, dst = ((cs_vmem, cs_hbm), (fe_vmem, fe_hbm))[which]
        rows = pl.ds(i * W, W)
        return pltpu.make_async_copy(src.at[:, rows], dst.at[:, rows], sem.at[which, i])

    for i in range(CHUNKS):
        put(0, i).start()
        put(1, i).start()
    for i in range(CHUNKS):
        put(0, i).wait()
        put(1, i).wait()


def local(sizes, field_values, mobility, source):
    J, I, K, L = field_values.shape
    f32 = jnp.float32
    vmem = pl.BlockSpec(memory_space=pltpu.VMEM)
    any_space = pl.BlockSpec(memory_space=pl.ANY)
    dma = pltpu.SemaphoreType.DMA
    column_sum, field_end = pl.pallas_call(
        functools.partial(kernel, (J, I, K, L), sizes),
        out_shape=[pltpu.VMEM((J, I, K, L), f32)] * 2,
        in_specs=[any_space] * 3,
        out_specs=[vmem] * 2,
        scratch_shapes=[
            pltpu.VMEM((2, J, I + 2, K, L), f32),
            pltpu.VMEM((2, I, K, L), f32),
            pltpu.VMEM((I, K, L), f32),
            pltpu.VMEM((2, 2, J, I, L), f32),
            pltpu.VMEM((2, 2, J, I, L), f32),
            dma((3, CHUNKS)),
            dma((2, CHUNKS)),
            dma((2, CHUNKS)),
            dma((STEPS, 2)),
            dma((STEPS, 2)),
            dma((2, 2, CHUNKS)),
            dma((2, 2, CHUNKS)),
        ],
        compiler_params=pltpu.CompilerParams(
            collective_id=0, has_side_effects=True, vmem_limit_bytes=32 * 1024 * 1024),
        name="diffuse",
    )(field_values, mobility, source)
    return tuple(pl.pallas_call(
        write_out,
        out_shape=[jax.ShapeDtypeStruct((J, I, K, L), f32)] * 2,
        in_specs=[vmem] * 2,
        out_specs=[any_space] * 2,
        scratch_shapes=[dma((2, CHUNKS))],
        compiler_params=pltpu.CompilerParams(vmem_limit_bytes=1024 * 1024),
        name="write_out",
    )(column_sum, field_end))


def solution(mesh):
    spec = P("rows", "cols", "slabs", None)
    sizes = tuple(mesh.shape[axis] for axis in ("rows", "cols", "slabs"))
    return jax.shard_map(functools.partial(local, sizes), mesh=mesh,
                         in_specs=(spec,) * 3, out_specs=(spec,) * 2, check_vma=False)
```

```python
import functools

import jax
import jax.numpy as jnp
from jax import lax
from jax.experimental import pallas as pl
from jax.experimental.pallas import tpu as pltpu
from jax.sharding import PartitionSpec as P

STEPS = 4
CHUNKS = 16
FIRST = 6
RELAYED = 6
MESH = pl.DeviceIdType.MESH


def kernel(dims, sizes, f_hbm, m_hbm, s_hbm, M, S, F, R, T, B, KS, KR,
           ld_sem, e_send, e_recv, h_send, h_recv, k_send, k_recv, r_send, r_recv, f_send):
    J, I, K, L = dims
    n_rows, n_cols, n_slabs = sizes
    W = I // CHUNKS
    r = lax.axis_index("rows")
    c = lax.axis_index("cols")
    s = lax.axis_index("slabs")
    other = 1 - r
    flip = c + 1 - 2 * (c % 2)
    edge = (J - 1) * (1 - r)
    edge_in = (J - 2) * (1 - r) + r
    far = (J - 1) * r
    far_in = (1 - r) + (J - 2) * r
    has_low, has_high = c > 0, c < n_cols - 1
    has_front, has_back = s > 0, s < n_slabs - 1

    def rows_of(chunk, extra=0):
        return pl.ds(chunk * W + extra, W)

    def edge_rows(t, chunk):
        if t == 0:
            return f_hbm.at[edge, rows_of(chunk)]
        if t < STEPS:
            return F.at[t % 2, edge, rows_of(chunk, 1)]
        return T.at[rows_of(chunk)]

    def e_copy(t, chunk):
        return pltpu.make_async_remote_copy(
            src_ref=edge_rows(t, chunk), dst_ref=R.at[t % 2, rows_of(chunk)],
            send_sem=e_send.at[t % 2, chunk], recv_sem=e_recv.at[t % 2, chunk],
            device_id={"rows": other}, device_id_type=MESH)

    def r_copy(i):
        return pltpu.make_async_remote_copy(
            src_ref=T.at[rows_of(FIRST + i)], dst_ref=B.at[i],
            send_sem=r_send.at[i], recv_sem=r_recv.at[i],
            device_id={"rows": other, "cols": flip}, device_id_type=MESH)

    def f_copy(i):
        return pltpu.make_async_remote_copy(
            src_ref=B.at[i], dst_ref=R.at[STEPS % 2, rows_of(FIRST + i)],
            send_sem=f_send.at[i], recv_sem=e_recv.at[STEPS % 2, FIRST + i],
            device_id={"cols": flip}, device_id_type=MESH)

    def h_copy(t, up):
        row = I - 1 if up else 0
        src = f_hbm.at[:, row] if t == 0 else F.at[t % 2, :, row + 1]
        return pltpu.make_async_remote_copy(
            src_ref=src, dst_ref=F.at[t % 2, :, 0 if up else I + 1],
            send_sem=h_send.at[t, up], recv_sem=h_recv.at[t, up],
            device_id={"cols": c + 1 if up else c - 1}, device_id_type=MESH)

    def k_copy(t, up, chunk):
        return pltpu.make_async_remote_copy(
            src_ref=KS.at[t % 2, up, :, rows_of(chunk)], dst_ref=KR.at[t % 2, up, :, rows_of(chunk)],
            send_sem=k_send.at[t % 2, up, chunk], recv_sem=k_recv.at[t % 2, up, chunk],
            device_id={"slabs": s + 1 if up else s - 1}, device_id_type=MESH)

    def load(which, chunk):
        hbm = (f_hbm, m_hbm, s_hbm)[which]
        dst = (F.at[0, :, rows_of(chunk, 1)], M.at[:, rows_of(chunk)], S.at[:, rows_of(chunk)])[which]
        return pltpu.make_async_copy(hbm.at[:, rows_of(chunk)], dst, ld_sem.at[which, chunk])

    def loop(n, body):
        def step(i, carry):
            body(i)
            return carry
        lax.fori_loop(0, n, step, 0)

    def span(start, stop, body):
        loop(stop - start, lambda i: body(start + i))

    barrier = pltpu.get_barrier_semaphore()
    greet = [(None, {"rows": other}), (None, {"rows": other, "cols": flip}),
             (has_low, {"cols": c - 1}), (has_high, {"cols": c + 1}),
             (has_front, {"slabs": s - 1}), (has_back, {"slabs": s + 1})]
    for cond, target in greet:
        def signal(target=target):
            pl.semaphore_signal(barrier, inc=1, device_id=target, device_id_type=MESH)
        signal() if cond is None else pl.when(cond)(signal)
    loop(CHUNKS, lambda i: load(0, i).start())
    peers = (2 + (c + n_cols - 1) // n_cols + (2 * n_cols - 2 - c) // n_cols
             + (s + n_slabs - 1) // n_slabs + (2 * n_slabs - 2 - s) // n_slabs)
    pl.semaphore_wait(barrier, peers)

    pl.when(has_high)(lambda: h_copy(0, 1).start())
    pl.when(has_low)(lambda: h_copy(0, 0).start())
    span(FIRST, CHUNKS, lambda i: e_copy(0, i).start())
    span(0, FIRST, lambda i: e_copy(0, i).start())

    for which in (1, 2):
        loop(CHUNKS, lambda i: load(which, i).start())

    zero_row = jnp.zeros((K, L), jnp.float32)
    for cond, row in ((c == 0, 0), (c == n_cols - 1, I + 1)):
        @pl.when(cond)
        def _():
            for slot in range(2):
                for p in range(J):
                    F[slot, p, row] = zero_row
    for cond, up in ((s == 0, 1), (s == n_slabs - 1, 0)):
        @pl.when(cond)
        def _():
            for slot in range(2):
                for p in range(J):
                    KR[slot, up, p] = jnp.zeros((I, L), jnp.float32)

    def send_faces(t, chunk):
        pl.when(has_front)(lambda: k_copy(t, 0, chunk).start())
        pl.when(has_back)(lambda: k_copy(t, 1, chunk).start())

    loop(CHUNKS, lambda i: load(0, i).wait())

    def first_faces(chunk):
        for p in range(J):
            def one(i, p=p):
                row = chunk * W + i
                x = F[0, p, row + 1]
                KS[0, 0, p, pl.ds(row, 1), :] = x[0:1]
                KS[0, 1, p, pl.ds(row, 1), :] = x[K - 1:K]
            loop(W, one)
        send_faces(0, chunk)
    span(FIRST, CHUNKS, first_faces)
    span(0, FIRST, first_faces)

    k_index = lax.broadcasted_iota(jnp.int32, (K, L), 0)

    def stencil_row(t, p, row, near):
        now, later = t % 2, (t + 1) % 2
        x = F[now, p, row + 1]
        below = jnp.where(k_index == 0, KR[now, 1, p, pl.ds(row, 1), :], pltpu.roll(x, 1, 0))
        above = jnp.where(k_index == K - 1, KR[now, 0, p, pl.ds(row, 1), :], pltpu.roll(x, K - 1, 0))
        total = near(row) + (F[now, p, row] + F[now, p, row + 2]) + (below + above) - 6.0 * x
        y = x + M[p, row] * total + S[p, row]
        if t == STEPS - 1:
            S[p, row] = y
        else:
            F[later, p, row + 1] = y
        if t < STEPS - 1:
            KS[later, 0, p, pl.ds(row, 1), :] = y[0:1]
            KS[later, 1, p, pl.ds(row, 1), :] = y[K - 1:K]

    def send_halo(t, up):
        pl.when(has_high if up else has_low)(lambda: h_copy(t, up).start())

    def step_chunk(t, chunk, totals=None):
        now = t % 2
        if t == 0:
            load(1, chunk).wait()
            load(2, chunk).wait()
        first, last = chunk == 0, chunk == CHUNKS - 1
        e_copy(t, chunk).wait_recv()
        pl.when(has_front)(lambda: k_copy(t, 1, chunk).wait_recv())
        pl.when(has_back)(lambda: k_copy(t, 0, chunk).wait_recv())
        pl.when(first & has_low)(lambda: h_copy(t, 1).wait_recv())
        pl.when(last & has_high)(lambda: h_copy(t, 0).wait_recv())
        if t > 0:
            pl.when(first & has_low)(lambda: h_copy(t - 1, 0).wait_send())
            pl.when(last & has_high)(lambda: h_copy(t - 1, 1).wait_send())
            pl.when(has_front)(lambda: k_copy(t - 1, 0, chunk).wait_send())
            pl.when(has_back)(lambda: k_copy(t - 1, 1, chunk).wait_send())
            e_copy(t - 1, chunk).wait_send()
        base = chunk * W
        loop(W, lambda i: stencil_row(
            t, edge, base + i, lambda row: F[now, edge_in, row + 1] + R[now, row]))
        if t < STEPS - 1:
            e_copy(t + 1, chunk).start()
        loop(W, lambda i: stencil_row(
            t, far, base + i, lambda row: F[now, far_in, row + 1]))
        for p in range(1, J - 1):
            loop(W, lambda i, p=p: stencil_row(
                t, p, base + i, lambda row: F[now, p - 1, row + 1] + F[now, p + 1, row + 1]))
        if t < STEPS - 1:
            if t > 0:
                pl.when(first)(lambda: send_halo(t + 1, 0))
                pl.when(last)(lambda: send_halo(t + 1, 1))
            send_faces(t + 1, chunk)
        else:
            @pl.when(r == 0)
            def _():
                def sums(i):
                    row = base + i
                    total = S[0, row]
                    M[0, row] = total * (1.0 / (J * n_rows))
                    for p in range(1, J):
                        total = total + S[p, row]
                        M[p, row] = total * (1.0 / (J * n_rows))
                    T[row] = total
                loop(W, sums)
                if totals == "relay":
                    r_copy(chunk - FIRST).start()
                elif totals == "direct":
                    e_copy(STEPS, chunk).start()

    def send_totals(*chunks):
        @pl.when(r == 0)
        def _():
            for chunk in chunks:
                e_copy(STEPS, chunk).start()

    def hand_on(start, stop):
        @pl.when(r == 1)
        def _():
            def one(i):
                r_copy(i).wait_recv()
                f_copy(i).start()
            span(start, stop, one)

    def both_ends(t, a, totals=None):
        loop(2, lambda i: step_chunk(t, a + i * (CHUNKS - 1 - 2 * a), totals))

    for t in range(STEPS - 1):
        span(FIRST, CHUNKS - t, lambda chunk: step_chunk(t, chunk))
        span(t, FIRST, lambda chunk: step_chunk(t, chunk))
    send_halo(1, 0)
    send_halo(1, 1)
    t = STEPS - 1
    after = FIRST + RELAYED
    span(FIRST, after, lambda chunk: step_chunk(t, chunk, "relay"))
    span(after, CHUNKS - t, lambda chunk: step_chunk(t, chunk))
    span(t, FIRST, lambda chunk: step_chunk(t, chunk))
    held = list(range(after, CHUNKS - t)) + list(range(t, FIRST))
    both_ends(1, 0)
    send_totals(*held[:2])
    both_ends(2, 1)
    both_ends(2, 0)
    send_totals(*held[2:])
    both_ends(3, 2, "direct")
    hand_on(0, RELAYED // 2)
    both_ends(3, 1, "direct")
    both_ends(3, 0, "direct")
    hand_on(RELAYED // 2, RELAYED)

    @pl.when(r == 0)
    def _():
        for chunk in range(CHUNKS):
            if not FIRST <= chunk < after:
                e_copy(STEPS, chunk).wait_send()
        for i in range(RELAYED):
            r_copy(i).wait_send()

    @pl.when(r == 1)
    def _():
        def finish(chunk):
            e_copy(STEPS, chunk).wait_recv()

            def sums(i):
                row = chunk * W + i
                total = R[STEPS % 2, row]
                for p in range(J):
                    total = total + S[p, row]
                    M[p, row] = total * (1.0 / (J * n_rows))
            loop(W, sums)
        span(after, CHUNKS - t, finish)
        span(t, FIRST, finish)
        for a in (2, 1):
            loop(2, lambda i: finish(a + i * (CHUNKS - 1 - 2 * a)))
        span(FIRST, after, finish)
        loop(2, lambda i: finish(i * (CHUNKS - 1)))
        for i in range(RELAYED):
            f_copy(i).wait_send()

    pl.when(has_low)(lambda: h_copy(STEPS - 1, 0).wait_send())
    pl.when(has_high)(lambda: h_copy(STEPS - 1, 1).wait_send())

    def drain(i):
        e_copy(STEPS - 1, i).wait_send()
        pl.when(has_front)(lambda: k_copy(STEPS - 1, 0, i).wait_send())
        pl.when(has_back)(lambda: k_copy(STEPS - 1, 1, i).wait_send())
    loop(CHUNKS, drain)


def write_out(cs_vmem, fe_vmem, cs_hbm, fe_hbm, sem):
    W = cs_vmem.shape[1] // CHUNKS

    def put(which, i):
        src, dst = ((cs_vmem, cs_hbm), (fe_vmem, fe_hbm))[which]
        rows = pl.ds(i * W, W)
        return pltpu.make_async_copy(src.at[:, rows], dst.at[:, rows], sem.at[which, i])

    for i in range(CHUNKS):
        put(0, i).start()
        put(1, i).start()
    for i in range(CHUNKS):
        put(0, i).wait()
        put(1, i).wait()


def local(sizes, field_values, mobility, source):
    J, I, K, L = field_values.shape
    f32 = jnp.float32
    vmem = pl.BlockSpec(memory_space=pltpu.VMEM)
    any_space = pl.BlockSpec(memory_space=pl.ANY)
    dma = pltpu.SemaphoreType.DMA
    column_sum, field_end = pl.pallas_call(
        functools.partial(kernel, (J, I, K, L), sizes),
        out_shape=[pltpu.VMEM((J, I, K, L), f32)] * 2,
        in_specs=[any_space] * 3,
        out_specs=[vmem] * 2,
        scratch_shapes=[
            pltpu.VMEM((2, J, I + 2, K, L), f32),
            pltpu.VMEM((2, I, K, L), f32),
            pltpu.VMEM((I, K, L), f32),
            pltpu.VMEM((RELAYED, I // CHUNKS, K, L), f32),
            pltpu.VMEM((2, 2, J, I, L), f32),
            pltpu.VMEM((2, 2, J, I, L), f32),
            dma((3, CHUNKS)),
            dma((2, CHUNKS)),
            dma((2, CHUNKS)),
            dma((STEPS, 2)),
            dma((STEPS, 2)),
            dma((2, 2, CHUNKS)),
            dma((2, 2, CHUNKS)),
            dma((RELAYED,)),
            dma((RELAYED,)),
            dma((RELAYED,)),
        ],
        compiler_params=pltpu.CompilerParams(
            collective_id=0, has_side_effects=True, vmem_limit_bytes=32 * 1024 * 1024),
        name="diffuse",
    )(field_values, mobility, source)
    return tuple(pl.pallas_call(
        write_out,
        out_shape=[jax.ShapeDtypeStruct((J, I, K, L), f32)] * 2,
        in_specs=[vmem] * 2,
        out_specs=[any_space] * 2,
        scratch_shapes=[dma((2, CHUNKS))],
        compiler_params=pltpu.CompilerParams(vmem_limit_bytes=1024 * 1024),
        name="write_out",
    )(column_sum, field_end))


def solution(mesh):
    spec = P("rows", "cols", "slabs", None)
    sizes = tuple(mesh.shape[axis] for axis in ("rows", "cols", "slabs"))
    return jax.shard_map(functools.partial(local, sizes), mesh=mesh,
                         in_specs=(spec,) * 3, out_specs=(spec,) * 2, check_vma=False)
```

```python
import functools

import jax
import jax.numpy as jnp
from jax import lax
from jax.experimental import pallas as pl
from jax.experimental.pallas import tpu as pltpu
from jax.sharding import PartitionSpec as P

STEPS = 4
CHUNKS = 16
FIRST = 5
RELAYED = 7
MESH = pl.DeviceIdType.MESH


def kernel(dims, sizes, f_hbm, m_hbm, s_hbm, M, S, F, R, T, B, KS, KR,
           ld_sem, e_send, e_recv, h_send, h_recv, k_send, k_recv, r_send, r_recv, f_send):
    J, I, K, L = dims
    n_rows, n_cols, n_slabs = sizes
    W = I // CHUNKS
    r = lax.axis_index("rows")
    c = lax.axis_index("cols")
    s = lax.axis_index("slabs")
    other = 1 - r
    flip = c + 1 - 2 * (c % 2)
    edge = (J - 1) * (1 - r)
    edge_in = (J - 2) * (1 - r) + r
    far = (J - 1) * r
    far_in = (1 - r) + (J - 2) * r
    has_low, has_high = c > 0, c < n_cols - 1
    has_front, has_back = s > 0, s < n_slabs - 1

    def rows_of(chunk, extra=0):
        return pl.ds(chunk * W + extra, W)

    def edge_rows(t, chunk):
        if t == 0:
            return f_hbm.at[edge, rows_of(chunk)]
        if t < STEPS:
            return F.at[t % 2, edge, rows_of(chunk, 1)]
        return T.at[rows_of(chunk)]

    def e_copy(t, chunk):
        return pltpu.make_async_remote_copy(
            src_ref=edge_rows(t, chunk), dst_ref=R.at[t % 2, rows_of(chunk)],
            send_sem=e_send.at[t % 2, chunk], recv_sem=e_recv.at[t % 2, chunk],
            device_id={"rows": other}, device_id_type=MESH)

    def r_copy(i):
        return pltpu.make_async_remote_copy(
            src_ref=T.at[rows_of(FIRST + i)], dst_ref=B.at[i],
            send_sem=r_send.at[i], recv_sem=r_recv.at[i],
            device_id={"rows": other, "cols": flip}, device_id_type=MESH)

    def f_copy(i):
        return pltpu.make_async_remote_copy(
            src_ref=B.at[i], dst_ref=R.at[STEPS % 2, rows_of(FIRST + i)],
            send_sem=f_send.at[i], recv_sem=e_recv.at[STEPS % 2, FIRST + i],
            device_id={"cols": flip}, device_id_type=MESH)

    def h_copy(t, up):
        row = I - 1 if up else 0
        src = f_hbm.at[:, row] if t == 0 else F.at[t % 2, :, row + 1]
        return pltpu.make_async_remote_copy(
            src_ref=src, dst_ref=F.at[t % 2, :, 0 if up else I + 1],
            send_sem=h_send.at[t, up], recv_sem=h_recv.at[t, up],
            device_id={"cols": c + 1 if up else c - 1}, device_id_type=MESH)

    def k_copy(t, up, chunk):
        return pltpu.make_async_remote_copy(
            src_ref=KS.at[t % 2, up, :, rows_of(chunk)], dst_ref=KR.at[t % 2, up, :, rows_of(chunk)],
            send_sem=k_send.at[t % 2, up, chunk], recv_sem=k_recv.at[t % 2, up, chunk],
            device_id={"slabs": s + 1 if up else s - 1}, device_id_type=MESH)

    def load(which, chunk):
        hbm = (f_hbm, m_hbm, s_hbm)[which]
        dst = (F.at[0, :, rows_of(chunk, 1)], M.at[:, rows_of(chunk)], S.at[:, rows_of(chunk)])[which]
        return pltpu.make_async_copy(hbm.at[:, rows_of(chunk)], dst, ld_sem.at[which, chunk])

    def loop(n, body):
        def step(i, carry):
            body(i)
            return carry
        lax.fori_loop(0, n, step, 0)

    def span(start, stop, body):
        loop(stop - start, lambda i: body(start + i))

    barrier = pltpu.get_barrier_semaphore()
    greet = [(None, {"rows": other}), (None, {"rows": other, "cols": flip}),
             (has_low, {"cols": c - 1}), (has_high, {"cols": c + 1}),
             (has_front, {"slabs": s - 1}), (has_back, {"slabs": s + 1})]
    for cond, target in greet:
        def signal(target=target):
            pl.semaphore_signal(barrier, inc=1, device_id=target, device_id_type=MESH)
        signal() if cond is None else pl.when(cond)(signal)
    loop(CHUNKS, lambda i: load(0, i).start())
    peers = (2 + (c + n_cols - 1) // n_cols + (2 * n_cols - 2 - c) // n_cols
             + (s + n_slabs - 1) // n_slabs + (2 * n_slabs - 2 - s) // n_slabs)
    pl.semaphore_wait(barrier, peers)

    span(FIRST, CHUNKS, lambda i: e_copy(0, i).start())
    span(0, FIRST, lambda i: e_copy(0, i).start())

    for which in (1, 2):
        loop(CHUNKS, lambda i: load(which, i).start())

    zero_row = jnp.zeros((K, L), jnp.float32)
    for cond, row in ((c == 0, 0), (c == n_cols - 1, I + 1)):
        @pl.when(cond)
        def _():
            for slot in range(2):
                for p in range(J):
                    F[slot, p, row] = zero_row
    for cond, up in ((s == 0, 1), (s == n_slabs - 1, 0)):
        @pl.when(cond)
        def _():
            for slot in range(2):
                for p in range(J):
                    KR[slot, up, p] = jnp.zeros((I, L), jnp.float32)

    def send_faces(t, chunk):
        pl.when(has_front)(lambda: k_copy(t, 0, chunk).start())
        pl.when(has_back)(lambda: k_copy(t, 1, chunk).start())

    loop(CHUNKS, lambda i: load(0, i).wait())

    def first_faces(chunk):
        for p in range(J):
            def one(i, p=p):
                row = chunk * W + i
                x = F[0, p, row + 1]
                KS[0, 0, p, pl.ds(row, 1), :] = x[0:1]
                KS[0, 1, p, pl.ds(row, 1), :] = x[K - 1:K]
            loop(W, one)
        send_faces(0, chunk)
    span(FIRST, CHUNKS, first_faces)
    span(0, FIRST, first_faces)

    k_index = lax.broadcasted_iota(jnp.int32, (K, L), 0)

    def stencil_row(t, p, row, near):
        now, later = t % 2, (t + 1) % 2
        x = F[now, p, row + 1]
        below = jnp.where(k_index == 0, KR[now, 1, p, pl.ds(row, 1), :], pltpu.roll(x, 1, 0))
        above = jnp.where(k_index == K - 1, KR[now, 0, p, pl.ds(row, 1), :], pltpu.roll(x, K - 1, 0))
        total = near(row) + (F[now, p, row] + F[now, p, row + 2]) + (below + above) - 6.0 * x
        y = x + M[p, row] * total + S[p, row]
        if t == STEPS - 1:
            S[p, row] = y
        else:
            F[later, p, row + 1] = y
        if t < STEPS - 1:
            KS[later, 0, p, pl.ds(row, 1), :] = y[0:1]
            KS[later, 1, p, pl.ds(row, 1), :] = y[K - 1:K]

    def send_halo(t, up):
        pl.when(has_high if up else has_low)(lambda: h_copy(t, up).start())

    def step_chunk(t, chunk, totals=None):
        now = t % 2
        if t == 0:
            load(1, chunk).wait()
            load(2, chunk).wait()
        first, last = chunk == 0, chunk == CHUNKS - 1
        e_copy(t, chunk).wait_recv()
        pl.when(has_front)(lambda: k_copy(t, 1, chunk).wait_recv())
        pl.when(has_back)(lambda: k_copy(t, 0, chunk).wait_recv())
        pl.when(first & has_low)(lambda: h_copy(t, 1).wait_recv())
        pl.when(last & has_high)(lambda: h_copy(t, 0).wait_recv())
        if t > 0:
            pl.when(first & has_low)(lambda: h_copy(t - 1, 0).wait_send())
            pl.when(last & has_high)(lambda: h_copy(t - 1, 1).wait_send())
            pl.when(has_front)(lambda: k_copy(t - 1, 0, chunk).wait_send())
            pl.when(has_back)(lambda: k_copy(t - 1, 1, chunk).wait_send())
            e_copy(t - 1, chunk).wait_send()
        base = chunk * W
        loop(W, lambda i: stencil_row(
            t, edge, base + i, lambda row: F[now, edge_in, row + 1] + R[now, row]))
        if t < STEPS - 1:
            e_copy(t + 1, chunk).start()
        loop(W, lambda i: stencil_row(
            t, far, base + i, lambda row: F[now, far_in, row + 1]))
        for p in range(1, J - 1):
            loop(W, lambda i, p=p: stencil_row(
                t, p, base + i, lambda row: F[now, p - 1, row + 1] + F[now, p + 1, row + 1]))
        if t < STEPS - 1:
            pl.when(first)(lambda: send_halo(t + 1, 0))
            pl.when(last)(lambda: send_halo(t + 1, 1))
            send_faces(t + 1, chunk)
        else:
            @pl.when(r == 0)
            def _():
                def sums(i):
                    row = base + i
                    total = S[0, row]
                    M[0, row] = total * (1.0 / (J * n_rows))
                    for p in range(1, J):
                        total = total + S[p, row]
                        M[p, row] = total * (1.0 / (J * n_rows))
                    T[row] = total
                loop(W, sums)
                if totals == "relay":
                    r_copy(chunk - FIRST).start()
                elif totals == "direct":
                    e_copy(STEPS, chunk).start()

    def send_totals(*chunks):
        @pl.when(r == 0)
        def _():
            for chunk in chunks:
                e_copy(STEPS, chunk).start()

    def hand_on(start, stop):
        @pl.when(r == 1)
        def _():
            def one(i):
                r_copy(i).wait_recv()
                f_copy(i).start()
            span(start, stop, one)

    def both_ends(t, a, totals=None):
        loop(2, lambda i: step_chunk(t, a + i * (CHUNKS - 1 - 2 * a), totals))

    for t in range(STEPS - 1):
        span(FIRST, CHUNKS - 1 - t, lambda chunk: step_chunk(t, chunk))
        span(t + 1, FIRST, lambda chunk: step_chunk(t, chunk))
    send_halo(0, 0)
    send_halo(0, 1)
    t = STEPS - 1
    after = FIRST + RELAYED
    span(FIRST, after, lambda chunk: step_chunk(t, chunk, "relay"))
    span(after, CHUNKS - STEPS, lambda chunk: step_chunk(t, chunk))
    span(STEPS, FIRST, lambda chunk: step_chunk(t, chunk))
    held = list(range(after, CHUNKS - STEPS)) + list(range(STEPS, FIRST))
    for begin in range(STEPS):
        for t in range(begin, STEPS):
            both_ends(t, t - begin, "direct")
            if t == begin == 2:
                send_totals(*held)
            if (begin, t) == (1, 3):
                hand_on(0, RELAYED // 2)
            if (begin, t) == (2, 3):
                hand_on(RELAYED // 2, RELAYED)

    @pl.when(r == 0)
    def _():
        for chunk in range(CHUNKS):
            if not FIRST <= chunk < after:
                e_copy(STEPS, chunk).wait_send()
        for i in range(RELAYED):
            r_copy(i).wait_send()

    @pl.when(r == 1)
    def _():
        def finish(chunk):
            e_copy(STEPS, chunk).wait_recv()

            def sums(i):
                row = chunk * W + i
                total = R[STEPS % 2, row]
                for p in range(J):
                    total = total + S[p, row]
                    M[p, row] = total * (1.0 / (J * n_rows))
            loop(W, sums)
        for a in (3, 2, 1):
            loop(2, lambda i: finish(a + i * (CHUNKS - 1 - 2 * a)))
        span(after, CHUNKS - STEPS, finish)
        span(STEPS, FIRST, finish)
        span(FIRST, after, finish)
        loop(2, lambda i: finish(i * (CHUNKS - 1)))
        for i in range(RELAYED):
            f_copy(i).wait_send()

    pl.when(has_low)(lambda: h_copy(STEPS - 1, 0).wait_send())
    pl.when(has_high)(lambda: h_copy(STEPS - 1, 1).wait_send())

    def drain(i):
        e_copy(STEPS - 1, i).wait_send()
        pl.when(has_front)(lambda: k_copy(STEPS - 1, 0, i).wait_send())
        pl.when(has_back)(lambda: k_copy(STEPS - 1, 1, i).wait_send())
    loop(CHUNKS, drain)


def write_out(cs_vmem, fe_vmem, cs_hbm, fe_hbm, sem):
    W = cs_vmem.shape[1] // CHUNKS

    def put(which, i):
        src, dst = ((cs_vmem, cs_hbm), (fe_vmem, fe_hbm))[which]
        rows = pl.ds(i * W, W)
        return pltpu.make_async_copy(src.at[:, rows], dst.at[:, rows], sem.at[which, i])

    for i in range(CHUNKS):
        put(0, i).start()
        put(1, i).start()
    for i in range(CHUNKS):
        put(0, i).wait()
        put(1, i).wait()


def local(sizes, field_values, mobility, source):
    J, I, K, L = field_values.shape
    f32 = jnp.float32
    vmem = pl.BlockSpec(memory_space=pltpu.VMEM)
    any_space = pl.BlockSpec(memory_space=pl.ANY)
    dma = pltpu.SemaphoreType.DMA
    column_sum, field_end = pl.pallas_call(
        functools.partial(kernel, (J, I, K, L), sizes),
        out_shape=[pltpu.VMEM((J, I, K, L), f32)] * 2,
        in_specs=[any_space] * 3,
        out_specs=[vmem] * 2,
        scratch_shapes=[
            pltpu.VMEM((2, J, I + 2, K, L), f32),
            pltpu.VMEM((2, I, K, L), f32),
            pltpu.VMEM((I, K, L), f32),
            pltpu.VMEM((RELAYED, I // CHUNKS, K, L), f32),
            pltpu.VMEM((2, 2, J, I, L), f32),
            pltpu.VMEM((2, 2, J, I, L), f32),
            dma((3, CHUNKS)),
            dma((2, CHUNKS)),
            dma((2, CHUNKS)),
            dma((STEPS, 2)),
            dma((STEPS, 2)),
            dma((2, 2, CHUNKS)),
            dma((2, 2, CHUNKS)),
            dma((RELAYED,)),
            dma((RELAYED,)),
            dma((RELAYED,)),
        ],
        compiler_params=pltpu.CompilerParams(
            collective_id=0, has_side_effects=True, vmem_limit_bytes=32 * 1024 * 1024),
        name="diffuse",
    )(field_values, mobility, source)
    return tuple(pl.pallas_call(
        write_out,
        out_shape=[jax.ShapeDtypeStruct((J, I, K, L), f32)] * 2,
        in_specs=[vmem] * 2,
        out_specs=[any_space] * 2,
        scratch_shapes=[dma((2, CHUNKS))],
        compiler_params=pltpu.CompilerParams(vmem_limit_bytes=1024 * 1024),
        name="write_out",
    )(column_sum, field_end))


def solution(mesh):
    spec = P("rows", "cols", "slabs", None)
    sizes = tuple(mesh.shape[axis] for axis in ("rows", "cols", "slabs"))
    return jax.shard_map(functools.partial(local, sizes), mesh=mesh,
                         in_specs=(spec,) * 3, out_specs=(spec,) * 2, check_vma=False)
```

```python
import functools

import jax
import jax.numpy as jnp
from jax import lax
from jax.experimental import pallas as pl
from jax.experimental.pallas import tpu as pltpu
from jax.sharding import PartitionSpec as P

STEPS = 4
CHUNKS = 16
FIRST = 5
RELAYED = 7
MESH = pl.DeviceIdType.MESH


def kernel(dims, sizes, f_hbm, m_hbm, s_hbm, M, S, F, R, T, B, KS, KR,
           ld_sem, e_send, e_recv, h_send, h_recv, k_send, k_recv, r_send, r_recv, f_send):
    J, I, K, L = dims
    n_rows, n_cols, n_slabs = sizes
    W = I // CHUNKS
    r = lax.axis_index("rows")
    c = lax.axis_index("cols")
    s = lax.axis_index("slabs")
    other = 1 - r
    flip = c + 1 - 2 * (c % 2)
    edge = (J - 1) * (1 - r)
    edge_in = (J - 2) * (1 - r) + r
    far = (J - 1) * r
    far_in = (1 - r) + (J - 2) * r
    has_low, has_high = c > 0, c < n_cols - 1
    has_front, has_back = s > 0, s < n_slabs - 1

    def rows_of(chunk, extra=0):
        return pl.ds(chunk * W + extra, W)

    def edge_rows(t, chunk):
        if t == 0:
            return f_hbm.at[edge, rows_of(chunk)]
        if t < STEPS:
            return F.at[t % 2, edge, rows_of(chunk, 1)]
        return T.at[rows_of(chunk)]

    def e_copy(t, chunk):
        return pltpu.make_async_remote_copy(
            src_ref=edge_rows(t, chunk), dst_ref=R.at[t % 2, rows_of(chunk)],
            send_sem=e_send.at[t % 2, chunk], recv_sem=e_recv.at[t % 2, chunk],
            device_id={"rows": other}, device_id_type=MESH)

    def r_copy(i):
        return pltpu.make_async_remote_copy(
            src_ref=T.at[rows_of(FIRST + i)], dst_ref=B.at[i],
            send_sem=r_send.at[i], recv_sem=r_recv.at[i],
            device_id={"rows": other, "cols": flip}, device_id_type=MESH)

    def f_copy(i):
        return pltpu.make_async_remote_copy(
            src_ref=B.at[i], dst_ref=R.at[STEPS % 2, rows_of(FIRST + i)],
            send_sem=f_send.at[i], recv_sem=e_recv.at[STEPS % 2, FIRST + i],
            device_id={"cols": flip}, device_id_type=MESH)

    def h_copy(t, up):
        row = I - 1 if up else 0
        src = f_hbm.at[:, row] if t == 0 else F.at[t % 2, :, row + 1]
        return pltpu.make_async_remote_copy(
            src_ref=src, dst_ref=F.at[t % 2, :, 0 if up else I + 1],
            send_sem=h_send.at[t, up], recv_sem=h_recv.at[t, up],
            device_id={"cols": c + 1 if up else c - 1}, device_id_type=MESH)

    def k_copy(t, up, chunk):
        return pltpu.make_async_remote_copy(
            src_ref=KS.at[t % 2, up, :, rows_of(chunk)], dst_ref=KR.at[t % 2, up, :, rows_of(chunk)],
            send_sem=k_send.at[t % 2, up, chunk], recv_sem=k_recv.at[t % 2, up, chunk],
            device_id={"slabs": s + 1 if up else s - 1}, device_id_type=MESH)

    def load(which, chunk):
        hbm = (f_hbm, m_hbm, s_hbm)[which]
        dst = (F.at[0, :, rows_of(chunk, 1)], M.at[:, rows_of(chunk)], S.at[:, rows_of(chunk)])[which]
        return pltpu.make_async_copy(hbm.at[:, rows_of(chunk)], dst, ld_sem.at[which, chunk])

    def loop(n, body):
        def step(i, carry):
            body(i)
            return carry
        lax.fori_loop(0, n, step, 0)

    def span(start, stop, body):
        loop(stop - start, lambda i: body(start + i))

    barrier = pltpu.get_barrier_semaphore()
    greet = [(None, {"rows": other}), (None, {"rows": other, "cols": flip}),
             (has_low, {"cols": c - 1}), (has_high, {"cols": c + 1}),
             (has_front, {"slabs": s - 1}), (has_back, {"slabs": s + 1})]
    for cond, target in greet:
        def signal(target=target):
            pl.semaphore_signal(barrier, inc=1, device_id=target, device_id_type=MESH)
        signal() if cond is None else pl.when(cond)(signal)
    loop(CHUNKS, lambda i: load(0, i).start())
    peers = (2 + (c + n_cols - 1) // n_cols + (2 * n_cols - 2 - c) // n_cols
             + (s + n_slabs - 1) // n_slabs + (2 * n_slabs - 2 - s) // n_slabs)
    pl.semaphore_wait(barrier, peers)

    span(FIRST, CHUNKS, lambda i: e_copy(0, i).start())
    span(0, FIRST, lambda i: e_copy(0, i).start())

    for which in (1, 2):
        loop(CHUNKS, lambda i: load(which, i).start())

    zero_row = jnp.zeros((K, L), jnp.float32)
    for cond, row in ((c == 0, 0), (c == n_cols - 1, I + 1)):
        @pl.when(cond)
        def _():
            for slot in range(2):
                for p in range(J):
                    F[slot, p, row] = zero_row
    for cond, up in ((s == 0, 1), (s == n_slabs - 1, 0)):
        @pl.when(cond)
        def _():
            for slot in range(2):
                for p in range(J):
                    KR[slot, up, p] = jnp.zeros((I, L), jnp.float32)

    def send_faces(t, chunk):
        pl.when(has_front)(lambda: k_copy(t, 0, chunk).start())
        pl.when(has_back)(lambda: k_copy(t, 1, chunk).start())

    loop(CHUNKS, lambda i: load(0, i).wait())

    def first_faces(chunk):
        for p in range(J):
            def one(i, p=p):
                row = chunk * W + i
                x = F[0, p, row + 1]
                KS[0, 0, p, pl.ds(row, 1), :] = x[0:1]
                KS[0, 1, p, pl.ds(row, 1), :] = x[K - 1:K]
            loop(W, one)
        send_faces(0, chunk)
    span(FIRST, CHUNKS, first_faces)
    span(0, FIRST, first_faces)

    k_index = lax.broadcasted_iota(jnp.int32, (K, L), 0)

    def stencil_row(t, p, row, near):
        now, later = t % 2, (t + 1) % 2
        x = F[now, p, row + 1]
        below = jnp.where(k_index == 0, KR[now, 1, p, pl.ds(row, 1), :], pltpu.roll(x, 1, 0))
        above = jnp.where(k_index == K - 1, KR[now, 0, p, pl.ds(row, 1), :], pltpu.roll(x, K - 1, 0))
        total = near(row) + (F[now, p, row] + F[now, p, row + 2]) + (below + above) - 6.0 * x
        y = x + M[p, row] * total + S[p, row]
        if t == STEPS - 1:
            S[p, row] = y
        else:
            F[later, p, row + 1] = y
        if t < STEPS - 1:
            KS[later, 0, p, pl.ds(row, 1), :] = y[0:1]
            KS[later, 1, p, pl.ds(row, 1), :] = y[K - 1:K]

    def send_halo(t, up):
        pl.when(has_high if up else has_low)(lambda: h_copy(t, up).start())

    def step_chunk(t, chunk, totals=None):
        now = t % 2
        if t == 0:
            load(1, chunk).wait()
            load(2, chunk).wait()
        first, last = chunk == 0, chunk == CHUNKS - 1
        e_copy(t, chunk).wait_recv()
        pl.when(has_front)(lambda: k_copy(t, 1, chunk).wait_recv())
        pl.when(has_back)(lambda: k_copy(t, 0, chunk).wait_recv())
        pl.when(first & has_low)(lambda: h_copy(t, 1).wait_recv())
        pl.when(last & has_high)(lambda: h_copy(t, 0).wait_recv())
        if t > 0:
            pl.when(first & has_low)(lambda: h_copy(t - 1, 0).wait_send())
            pl.when(last & has_high)(lambda: h_copy(t - 1, 1).wait_send())
            pl.when(has_front)(lambda: k_copy(t - 1, 0, chunk).wait_send())
            pl.when(has_back)(lambda: k_copy(t - 1, 1, chunk).wait_send())
            e_copy(t - 1, chunk).wait_send()
        base = chunk * W
        loop(W, lambda i: stencil_row(
            t, edge, base + i, lambda row: F[now, edge_in, row + 1] + R[now, row]))
        if t < STEPS - 1:
            e_copy(t + 1, chunk).start()
        loop(W, lambda i: stencil_row(
            t, far, base + i, lambda row: F[now, far_in, row + 1]))
        for p in range(1, J - 1):
            loop(W, lambda i, p=p: stencil_row(
                t, p, base + i, lambda row: F[now, p - 1, row + 1] + F[now, p + 1, row + 1]))
        if t < STEPS - 1:
            pl.when(first)(lambda: send_halo(t + 1, 0))
            pl.when(last)(lambda: send_halo(t + 1, 1))
            send_faces(t + 1, chunk)
        else:
            @pl.when(r == 0)
            def _():
                def sums(i):
                    row = base + i
                    total = S[0, row]
                    M[0, row] = total * (1.0 / (J * n_rows))
                    for p in range(1, J):
                        total = total + S[p, row]
                        M[p, row] = total * (1.0 / (J * n_rows))
                    T[row] = total
                loop(W, sums)
                if totals == "relay":
                    r_copy(chunk - FIRST).start()
                elif totals == "direct":
                    e_copy(STEPS, chunk).start()

    def send_totals(*chunks):
        @pl.when(r == 0)
        def _():
            for chunk in chunks:
                e_copy(STEPS, chunk).start()

    def hand_on(start, stop):
        @pl.when(r == 1)
        def _():
            def one(i):
                r_copy(i).wait_recv()
                f_copy(i).start()
            span(start, stop, one)

    def both_ends(t, a, totals=None):
        loop(2, lambda i: step_chunk(t, a + i * (CHUNKS - 1 - 2 * a), totals))

    for t in range(STEPS - 1):
        span(FIRST, CHUNKS - 1 - t, lambda chunk: step_chunk(t, chunk))
        span(t + 1, FIRST, lambda chunk: step_chunk(t, chunk))
    send_halo(0, 0)
    send_halo(0, 1)
    t = STEPS - 1
    after = FIRST + RELAYED
    span(FIRST, after, lambda chunk: step_chunk(t, chunk, "relay"))
    span(after, CHUNKS - STEPS, lambda chunk: step_chunk(t, chunk))
    span(STEPS, FIRST, lambda chunk: step_chunk(t, chunk))
    held = list(range(after, CHUNKS - STEPS)) + list(range(STEPS, FIRST))
    for begin in range(STEPS):
        for t in range(begin, STEPS):
            both_ends(t, t - begin, "direct")
            if t == begin == 2:
                send_totals(*held)
            if (begin, t) == (1, 3):
                hand_on(0, RELAYED // 2)
            if (begin, t) == (2, 3):
                hand_on(RELAYED // 2, RELAYED)

    @pl.when(r == 0)
    def _():
        for chunk in range(CHUNKS):
            if not FIRST <= chunk < after:
                e_copy(STEPS, chunk).wait_send()
        for i in range(RELAYED):
            r_copy(i).wait_send()

    @pl.when(r == 1)
    def _():
        def finish(chunk):
            e_copy(STEPS, chunk).wait_recv()

            def sums(i):
                row = chunk * W + i
                total = R[STEPS % 2, row]
                for p in range(J):
                    total = total + S[p, row]
                    M[p, row] = total * (1.0 / (J * n_rows))
            loop(W, sums)
        for a in (3, 2, 1):
            loop(2, lambda i: finish(a + i * (CHUNKS - 1 - 2 * a)))
        span(after, CHUNKS - STEPS, finish)
        span(STEPS, FIRST, finish)
        span(FIRST, after, finish)
        loop(2, lambda i: finish(i * (CHUNKS - 1)))
        for i in range(RELAYED):
            f_copy(i).wait_send()

    pl.when(has_low)(lambda: h_copy(STEPS - 1, 0).wait_send())
    pl.when(has_high)(lambda: h_copy(STEPS - 1, 1).wait_send())

    def drain(i):
        e_copy(STEPS - 1, i).wait_send()
        pl.when(has_front)(lambda: k_copy(STEPS - 1, 0, i).wait_send())
        pl.when(has_back)(lambda: k_copy(STEPS - 1, 1, i).wait_send())
    loop(CHUNKS, drain)


def write_out(cs_vmem, fe_vmem, cs_hbm, fe_hbm, sem):
    J, W = cs_vmem.shape[0], cs_vmem.shape[1] // CHUNKS

    def put(which, p, i):
        src, dst = ((cs_vmem, cs_hbm), (fe_vmem, fe_hbm))[which]
        rows = pl.ds(i * W, W)
        return pltpu.make_async_copy(src.at[p, rows], dst.at[p, rows], sem.at[which, p, i])

    pieces = [(which, p, i) for which in range(2) for p in range(J) for i in range(CHUNKS)]
    for piece in pieces:
        put(*piece).start()
    for piece in pieces:
        put(*piece).wait()


def local(sizes, field_values, mobility, source):
    J, I, K, L = field_values.shape
    f32 = jnp.float32
    vmem = pl.BlockSpec(memory_space=pltpu.VMEM)
    any_space = pl.BlockSpec(memory_space=pl.ANY)
    dma = pltpu.SemaphoreType.DMA
    column_sum, field_end = pl.pallas_call(
        functools.partial(kernel, (J, I, K, L), sizes),
        out_shape=[pltpu.VMEM((J, I, K, L), f32)] * 2,
        in_specs=[any_space] * 3,
        out_specs=[vmem] * 2,
        scratch_shapes=[
            pltpu.VMEM((2, J, I + 2, K, L), f32),
            pltpu.VMEM((2, I, K, L), f32),
            pltpu.VMEM((I, K, L), f32),
            pltpu.VMEM((RELAYED, I // CHUNKS, K, L), f32),
            pltpu.VMEM((2, 2, J, I, L), f32),
            pltpu.VMEM((2, 2, J, I, L), f32),
            dma((3, CHUNKS)),
            dma((2, CHUNKS)),
            dma((2, CHUNKS)),
            dma((STEPS, 2)),
            dma((STEPS, 2)),
            dma((2, 2, CHUNKS)),
            dma((2, 2, CHUNKS)),
            dma((RELAYED,)),
            dma((RELAYED,)),
            dma((RELAYED,)),
        ],
        compiler_params=pltpu.CompilerParams(
            collective_id=0, has_side_effects=True, vmem_limit_bytes=32 * 1024 * 1024),
        name="diffuse",
    )(field_values, mobility, source)
    return tuple(pl.pallas_call(
        write_out,
        out_shape=[jax.ShapeDtypeStruct((J, I, K, L), f32)] * 2,
        in_specs=[vmem] * 2,
        out_specs=[any_space] * 2,
        scratch_shapes=[dma((2, J, CHUNKS))],
        compiler_params=pltpu.CompilerParams(vmem_limit_bytes=1024 * 1024),
        name="write_out",
    )(column_sum, field_end))


def solution(mesh):
    spec = P("rows", "cols", "slabs", None)
    sizes = tuple(mesh.shape[axis] for axis in ("rows", "cols", "slabs"))
    return jax.shard_map(functools.partial(local, sizes), mesh=mesh,
                         in_specs=(spec,) * 3, out_specs=(spec,) * 2, check_vma=False)
```
